32 devices in a mesh: lat: 8 (over z, y), fld: 4 (over x, core).
Axes of the slice: x: 2, y: 2, z: 4, core: 2. Of those that a mesh axis runs over, the one named last changes fastest.
Arguments:
- grid_fields: bfloat16 [96, 1280, 2560], P('fld', 'lat'), may hold values from -6 to 6
- assign: int32 [320], replicated, may hold values from 0 to 319, each once
- limits: int32 [3], replicated, may hold values from 60 to 319, as said below
- legendre: bfloat16 [320, 641, 640], P('lat', None, 'fld'), may hold values from -0.25 to 0.25
- synth_one: bfloat16 [320, 320, 320], P('lat'), may hold values from -0.3125 to 0.3125
- synth_two: bfloat16 [320, 160, 160], P('lat'), may hold values from -0.5 to 0.5
- synth_three: bfloat16 [320, 80, 80], P('lat'), may hold values from -0.625 to 0.625
Outputs:
- spectrum: bfloat16 [96, 2, 320, 641], P('fld', None, 'lat')
- grid_one: float32 [96, 640, 1280], P('fld', 'lat')
- grid_two: float32 [96, 320, 640], P('fld', 'lat')
- grid_three: float32 [96, 160, 320], P('fld', 'lat')
The draws below stay inside these ranges and needn't reach their ends.
Inputs may be any that keep to these rules, and one draw needn't show every extreme that they name: assign is a permutation; slot q stands for the wavenumbers assign[q] and 639 - assign[q]. limits[0] is 319, limits[2] is 60, and limits[1] lies between 120 and 159.
All inputs are finite; a program needn't handle non-finite values.
Results may differ from the reference program's by a relative error of at most 0.0077.
Values may be sent and summed in bfloat16 or wider, within the bound.
A program may use at most 256 MiB of HBM per device.

```python
import math
import jax
import jax.numpy as jnp

MW = 640
NLAT = 1280
NLON = 2560
FIELDS = 96
PAIRS = 320
PACK = 641
NH = 640
MW1 = 320
MW2 = 160
MW3 = 80


def draw_limits(key, part):
    counts = jnp.array([MW // 2, MW // 4, MW // 8], dtype=jnp.int32)
    middle = jax.random.randint(key, (), 0, MW // 4 // 4, dtype=jnp.int32)
    offsets = jnp.stack([jnp.zeros((), jnp.int32), middle, jnp.full((), MW // 8 // 4, jnp.int32)])
    return counts - 1 - offsets + jnp.array([0, 0, 1], dtype=jnp.int32)


def level_of(own_key, extent, pieces, least, top_value):
    factor_of = 1.0
    for axis_at, parts in pieces:
        steps = jax.random.uniform(jax.random.fold_in(jax.random.fold_in(own_key, 6), axis_at), (parts,), jnp.float32, least / len(pieces), top_value / len(pieces))
        factor_of = factor_of * jnp.repeat(jnp.exp(steps), extent[axis_at] // parts).reshape((-1,) + (1,) * (len(extent) - 1 - axis_at))
    return factor_of


def centred(rng, shape, spread, reach, pieces=(), kind=jnp.bfloat16):
    values = spread * jax.random.normal(rng, shape, jnp.float32)
    if pieces:
        values = values * level_of(rng, shape, pieces, -0.22, 0.18)
    return jnp.clip(values, -reach, reach).astype(kind)


def setup_inputs(seed: int = 0) -> dict:
    splits = jax.random.split(jax.random.key(seed), 8)
    grid_fields = centred(splits[0], (FIELDS, NLAT, NLON), 1.0, 6.0, ((0, 4), (1, 8)))
    assign = jax.random.permutation(splits[1], PAIRS).astype(jnp.int32)
    limits = draw_limits(jax.random.fold_in(splits[7], 71), 0)
    legendre = centred(splits[3], (PAIRS, PACK, NH), NH ** -0.5, 0.25, ((0, 8), (2, 4)))
    synth_one = centred(splits[4], (PAIRS, MW1, MW1), MW1 ** -0.5, 0.3125, ((0, 8),))
    synth_two = centred(splits[5], (PAIRS, MW2, MW2), MW2 ** -0.5, 0.5, ((0, 8),))
    synth_three = centred(splits[6], (PAIRS, MW3, MW3), MW3 ** -0.5, 0.625, ((0, 8),))
    return dict(grid_fields=grid_fields, assign=assign, limits=limits, legendre=legendre, synth_one=synth_one, synth_two=synth_two, synth_three=synth_three)


def phases(lon_length, wavenums):
    places = jnp.arange(lon_length, dtype=jnp.int32)
    turn_count = places[:, None] * wavenums[None, :].astype(jnp.int32) % lon_length
    angle = turn_count.astype(jnp.float32) * (2.0 * math.pi / lon_length)
    return (jnp.cos(angle), jnp.sin(angle))

def choose_pair(values, limit_of):
    ranks = jnp.arange(values.shape[-1], dtype=jnp.int32)
    keep_mask = ranks[None, :] < limit_of[:, None]
    return jnp.where(keep_mask[None, None], values[:, :, :, 0], values[:, :, :, 1])

def select_rows(sym_prod, anti_prod, own_pairs, wave_total):
    first_rows = choose_pair(sym_prod, (wave_total + 1 - own_pairs) // 2)
    later_rows = choose_pair(anti_prod, (wave_total - own_pairs) // 2)
    return jnp.concatenate([first_rows, later_rows], axis=3)

def level_field(spectrum, own_pairs, limit, synth_table):
    half_rows = synth_table.shape[1] // 2
    sym_rows = spectrum.shape[3] // 2 + 1
    step_rows = 2 * jnp.arange(half_rows, dtype=jnp.int32)
    keep_sym = own_pairs[:, None] + step_rows[None, :] <= limit
    keep_anti = own_pairs[:, None] + 1 + step_rows[None, :] <= limit
    zero_value = jnp.zeros((), jnp.bfloat16)
    kept_sym = jnp.where(keep_sym[None, None], spectrum[..., :half_rows], zero_value)
    kept_anti = jnp.where(keep_anti[None, None], spectrum[..., sym_rows:sym_rows + half_rows], zero_value)
    even_part = jnp.einsum('fcqk,qkj->fcjq', kept_sym.astype(jnp.float32), synth_table[:, :half_rows].astype(jnp.float32))
    odd_part = jnp.einsum('fcqk,qkj->fcjq', kept_anti.astype(jnp.float32), synth_table[:, half_rows:].astype(jnp.float32))
    return jnp.concatenate([even_part + odd_part, jnp.flip(even_part - odd_part, axis=2)], axis=2).astype(jnp.bfloat16)

def inverse_table(assign, lon_length):
    cosine, sine_part = phases(lon_length, assign)
    weight = jnp.where(assign == 0, 1.0, 2.0).astype(jnp.float32) / math.sqrt(lon_length)
    return jnp.stack([cosine.T * weight[:, None], -sine_part.T * weight[:, None]], axis=0).astype(jnp.bfloat16)

def reference(grid_fields, assign, limits, legendre, synth_one, synth_two, synth_three):
    pair_total = assign.shape[0]
    wave_total = 2 * pair_total
    sym_rows = pair_total + 1
    field_count, lat_total, lon_total = grid_fields.shape
    half_lat = lat_total // 2
    wavenums = jnp.stack([assign, wave_total - 1 - assign], axis=1).reshape(-1)
    cosine, sine_part = phases(lon_total, wavenums)
    dft_scale = 1.0 / math.sqrt(lon_total)
    dft_table = jnp.stack([cosine * dft_scale, -sine_part * dft_scale], axis=1).reshape(lon_total, -1).astype(jnp.bfloat16)
    fourier = jnp.dot(grid_fields.reshape(-1, lon_total), dft_table, preferred_element_type=jnp.float32).astype(jnp.bfloat16)
    split_four = fourier.reshape(field_count, lat_total, 2, pair_total, 2).astype(jnp.float32)
    north_rows = split_four[:, :half_lat]
    south_rows = jnp.flip(split_four[:, half_lat:], axis=1)
    symmetric = (north_rows + south_rows).astype(jnp.bfloat16)
    antisym = (north_rows - south_rows).astype(jnp.bfloat16)
    sym_prod = jnp.einsum('kjcsw,srj->kcswr', symmetric.astype(jnp.float32), legendre[:, :sym_rows].astype(jnp.float32))
    anti_prod = jnp.einsum('kjcsw,srj->kcswr', antisym.astype(jnp.float32), legendre[:, sym_rows:].astype(jnp.float32))
    spectrum = select_rows(sym_prod, anti_prod, assign, wave_total).astype(jnp.bfloat16)
    grids_out = []
    for level_index, synth_table in enumerate((synth_one, synth_two, synth_three)):
        level_rows = level_field(spectrum, assign, limits[level_index], synth_table)
        inverse = inverse_table(assign, 4 * synth_table.shape[1])
        grids_out.append(jnp.einsum('fcjq,cqi->fji', level_rows.astype(jnp.float32), inverse.astype(jnp.float32)))
    return (spectrum, grids_out[0], grids_out[1], grids_out[2])
```

```python
import functools
import math

import jax
import jax.numpy as jnp
from jax import lax
from jax.experimental import pallas as pl
from jax.experimental.pallas import tpu as pltpu
from jax.sharding import PartitionSpec as P


CHUNKS = 1


def choose_pair(values, limit_of):
    ranks = jnp.arange(values.shape[-1], dtype=jnp.int32)
    keep_mask = ranks[None, :] < limit_of[:, None]
    return jnp.where(keep_mask[None, None], values[:, :, :, 0], values[:, :, :, 1])


def select_rows(sym_prod, anti_prod, own_pairs, wave_total):
    first_rows = choose_pair(sym_prod, (wave_total + 1 - own_pairs) // 2)
    later_rows = choose_pair(anti_prod, (wave_total - own_pairs) // 2)
    return jnp.concatenate([first_rows, later_rows], axis=3)


def level_rows_of(spectrum, own_pairs, limit, synth_table, lat_count):
    half_rows = synth_table.shape[1] // 2
    sym_rows = spectrum.shape[3] // 2 + 1
    step_rows = 2 * jnp.arange(half_rows, dtype=jnp.int32)
    keep_sym = own_pairs[:, None] + step_rows[None, :] <= limit
    keep_anti = own_pairs[:, None] + 1 + step_rows[None, :] <= limit
    zero_value = jnp.zeros((), jnp.bfloat16)
    kept_sym = jnp.where(keep_sym[None, None], spectrum[..., :half_rows], zero_value)
    kept_anti = jnp.where(
        keep_anti[None, None], spectrum[..., sym_rows : sym_rows + half_rows], zero_value
    )
    even_part = jnp.einsum(
        "fcqk,qkj->qcfj", kept_sym, synth_table[:, :half_rows], preferred_element_type=jnp.float32
    )
    odd_part = jnp.einsum(
        "fcqk,qkj->qcfj", kept_anti, synth_table[:, half_rows:], preferred_element_type=jnp.float32
    )
    north = (even_part + odd_part).astype(jnp.bfloat16)
    south = jnp.flip((even_part - odd_part).astype(jnp.bfloat16), axis=3)
    slots, parts, fields, half_lat = north.shape
    owners = lat_count // 2
    halves = [
        part.reshape(slots * parts, fields, owners, half_lat // owners)
        .transpose(2, 0, 1, 3)
        .reshape(owners, slots * parts, -1)
        for part in (north, south)
    ]
    return jnp.concatenate(halves, axis=0)


def quarter_of(values, axis):
    return lax.broadcasted_iota(jnp.int32, values.shape, axis).reshape(-1)


def turned_cosine(waves, quarters, places):
    length = places.shape[0]
    inner = 128 if length % 128 == 0 else math.gcd(length, 128)
    coarse = jnp.arange(length // inner, dtype=jnp.int32) * inner
    fine = jnp.arange(inner, dtype=jnp.int32)
    step = 2.0 * math.pi / length

    def angles(at, shift):
        return ((waves[:, None] * at[None, :] + shift) % length).astype(jnp.float32) * step

    outer_angle = angles(coarse, quarters[:, None] * (length // 4))
    inner_angle = angles(fine, 0)
    outer_cos, outer_sin = jnp.cos(outer_angle), jnp.sin(outer_angle)
    inner_cos, inner_sin = jnp.cos(inner_angle), jnp.sin(inner_angle)
    outer_cos, outer_sin, inner_cos, inner_sin = lax.optimization_barrier(
        (outer_cos, outer_sin, inner_cos, inner_sin)
    )
    pieces = [
        outer_cos[:, at : at + 1] * inner_cos - outer_sin[:, at : at + 1] * inner_sin
        for at in range(length // inner)
    ]
    return jnp.concatenate(pieces, axis=1)


def inverse_table(order, lon_length):
    waves = jnp.stack([order, order], axis=1)
    weight = jnp.where(waves == 0, 1.0, 2.0).astype(jnp.float32) / math.sqrt(lon_length)
    places = jnp.arange(lon_length, dtype=jnp.int32)
    table = turned_cosine(waves.reshape(-1), quarter_of(waves, 1), places)
    return (table * weight.reshape(-1)[:, None]).astype(jnp.bfloat16)


def plain_on_device(grid_fields, assign, limits, legendre, synth_one, synth_two, synth_three):
    lat_count = lax.axis_size("lat")
    field_count, row_count, lon_total = grid_fields.shape
    pair_total = assign.shape[0]
    pair_local = pair_total // lat_count
    wave_total = 2 * pair_total
    sym_rows = pair_total + 1
    chunks = CHUNKS
    while pair_local % chunks:
        chunks -= 1
    slots = pair_local // chunks
    half_count = lat_count // 2
    synth_tables = (synth_one, synth_two, synth_three)
    dft_scale = 1.0 / math.sqrt(lon_total)
    flat_grid = grid_fields.reshape(field_count * row_count, lon_total)
    by_owner = assign.reshape(lat_count, chunks, slots)
    own_all = lax.dynamic_index_in_dim(by_owner, lax.axis_index("lat"), 0, keepdims=False)

    places = jnp.arange(lon_total, dtype=jnp.int32)
    sent_rows = []
    gathered = []
    for at in range(chunks):
        own_block = legendre[at * slots : (at + 1) * slots]
        gathered.append(
            [
                lax.all_gather(part, "fld", axis=2, tiled=True)
                for part in (own_block[:, :sym_rows], own_block[:, sym_rows:])
            ]
        )
    for at in range(chunks):
        waves = jnp.stack([by_owner[:, at], wave_total - 1 - by_owner[:, at]], axis=2)
        waves = jnp.stack([waves, waves], axis=1)
        dft_table = (
            turned_cosine(waves.reshape(-1), quarter_of(waves, 1), places) * dft_scale
        ).astype(jnp.bfloat16)
        fourier = lax.dot_general(
            dft_table,
            flat_grid,
            (((1,), (1,)), ((), ())),
            preferred_element_type=jnp.float32,
        ).astype(jnp.bfloat16)
        sent_rows.append(
            lax.all_to_all(
                fourier.reshape(lat_count, 4 * slots, field_count * row_count),
                "lat",
                split_axis=0,
                concat_axis=0,
                tiled=True,
            )
        )

    spectra = []
    arrived = []
    for at in range(chunks):
        own_pairs = own_all[at]
        split_six = (
            sent_rows[at]
            .reshape(lat_count, 2, slots, 2, field_count, row_count)
            .transpose(2, 1, 3, 4, 0, 5)
        )
        flat_shape = (slots, 2, 2, field_count, half_count * row_count)
        split_six = lax.optimization_barrier(split_six)
        north_rows = split_six[..., :half_count, :].reshape(flat_shape).astype(jnp.float32)
        south_rows = jnp.flip(split_six[..., half_count:, :].reshape(flat_shape), axis=4).astype(
            jnp.float32
        )
        symmetric = (north_rows + south_rows).astype(jnp.bfloat16)
        antisym = (north_rows - south_rows).astype(jnp.bfloat16)
        block_piece = gathered[at]
        sym_add = jnp.einsum(
            "scwkj,srj->kcswr",
            symmetric,
            block_piece[0],
            preferred_element_type=jnp.float32,
        )
        anti_add = jnp.einsum(
            "scwkj,srj->kcswr",
            antisym,
            block_piece[1],
            preferred_element_type=jnp.float32,
        )
        spectrum = select_rows(sym_add, anti_add, own_pairs, wave_total).astype(jnp.bfloat16)
        spectra.append(spectrum)
        level_blocks = [
            level_rows_of(
                spectrum,
                own_pairs,
                limits[level],
                synth_tables[level][at * slots : (at + 1) * slots],
                lat_count,
            )
            for level in range(3)
        ]
        arrived.append(
            lax.all_to_all(
                jnp.concatenate(level_blocks, axis=2),
                "lat",
                split_axis=0,
                concat_axis=0,
                tiled=True,
            )
        )

    order = by_owner.transpose(1, 0, 2).reshape(-1)
    all_rows = jnp.stack(arrived, axis=0).reshape(2 * pair_total, -1)
    grids_out = []
    start = 0
    for level in range(3):
        level_lat = 2 * synth_tables[level].shape[1]
        own_rows = level_lat // lat_count
        width = field_count * own_rows
        inverse = inverse_table(order, 2 * level_lat)
        grids_out.append(
            lax.dot_general(
                all_rows[:, start : start + width],
                inverse,
                (((0,), (0,)), ((), ())),
                preferred_element_type=jnp.float32,
            ).reshape(field_count, own_rows, -1)
        )
        start += width
    return (jnp.concatenate(spectra, axis=2), grids_out[0], grids_out[1], grids_out[2])


F32 = jnp.float32
BF16 = jnp.bfloat16
LANES = 128
GROUP = 4
SLOTS = 8
VMEM_LIMIT = 56 * 1024 * 1024


def fits(grid_fields, assign, limits, legendre, synth_one, synth_two, synth_three):
    field_count, row_count, lon_total = grid_fields.shape
    lat_count = lax.axis_size("lat")
    pair_local = assign.shape[0] // lat_count
    rest = row_count - LANES
    counts = (synth_one.shape[1], synth_two.shape[1], synth_three.shape[1])
    owns = [2 * count // lat_count for count in counts]
    return (
        lat_count == 8
        and lax.axis_size("fld") * row_count == legendre.shape[2] * lax.axis_size("fld")
        and lax.axis_size("fld") == lat_count // 2
        and rest * GROUP == LANES
        and field_count == 6 * GROUP
        and lon_total % LANES == 0
        and pair_local % SLOTS == 0
        and legendre.shape[1] == 2 * assign.shape[0] + 1
        and (2 * assign.shape[0]) % LANES == 0
        and owns[0] % 16 == 0
        and owns[0] + owns[1] + 8 == LANES
        and 3 * owns[2] <= 64
        and counts[0] <= 384
        and counts[1] <= 256
        and counts[2] <= LANES
    )


def nt_dot(left, right):
    return lax.dot_general(left, right, (((1,), (1,)), ((), ())), preferred_element_type=F32)


def nn_dot(left, right):
    return jnp.dot(left, right, preferred_element_type=F32)


def eye_of(size):
    rows = lax.broadcasted_iota(jnp.int32, (size, size), 0)
    columns = lax.broadcasted_iota(jnp.int32, (size, size), 1)
    return jnp.where(rows == columns, 1.0, 0.0).astype(BF16)


def picks(rows, source):
    return jnp.where(rows == source, 1.0, 0.0).astype(BF16)


def dft_body(chunks, scale, shift_ref, ocos, osin, icos, isin, grid_ref, after_ref, *rest):
    outs, table, stage = rest[:8], rest[8], rest[9]
    per_slot = 2 * SLOTS
    side = 8 * per_slot
    coefs = 2 * side
    steps = ocos.shape[0]

    @pl.when(pl.program_id(0) == 0)
    def _():
        for at in range(chunks):
            lanes = slice(at * side, (at + 1) * side)
            cos_in, sin_in = icos[:, lanes] * scale, isin[:, lanes] * scale
            for step in range(steps):
                cos_out, sin_out = ocos[step : step + 1, lanes], osin[step : step + 1, lanes]
                rows = slice(step * LANES, (step + 1) * LANES)
                table[rows, at * coefs : at * coefs + side] = (
                    cos_out * cos_in - sin_out * sin_in
                ).astype(BF16)
                table[rows, at * coefs + side : (at + 1) * coefs] = (
                    -(sin_out * cos_in + cos_out * sin_in)
                ).astype(BF16)

    group, row_count, lon_total = grid_ref.shape
    small = row_count - LANES
    values = grid_ref[...].reshape(group * row_count, lon_total)
    first = pl.multiple_of(shift_ref[0], 16)
    second = pl.multiple_of(shift_ref[1], 16)
    eye = eye_of(coefs)
    for at in range(chunks):
        stage[...] = nn_dot(values, table[:, at * coefs : (at + 1) * coefs]).astype(BF16)
        pieces = [stage[pl.ds(f * row_count + first, LANES), :] for f in range(group)]
        pieces += [stage[pl.ds(f * row_count + second, small), :] for f in range(group)]
        turned = nt_dot(eye, jnp.concatenate(pieces, axis=0)).astype(BF16)
        for k in range(8):
            for c in range(2):
                start = c * side + k * per_slot
                for tile in range(group + 1):
                    outs[k][at, 0, tile, c * per_slot : (c + 1) * per_slot, :] = turned[
                        start : start + per_slot, tile * LANES : (tile + 1) * LANES
                    ]


def dft_call(shift, trig, grid_fields, after):
    ocos, osin, icos, isin = trig
    field_count, row_count, lon_total = grid_fields.shape
    chunks = ocos.shape[1] // (8 * 2 * SLOTS)
    coefs = 8 * 4 * SLOTS
    groups = field_count // GROUP
    whole = lambda shape: pl.BlockSpec(shape, lambda g, *_: (0,) * len(shape))
    out = jax.ShapeDtypeStruct((chunks, groups, GROUP + 1, 4 * SLOTS, LANES), BF16)
    return pl.pallas_call(
        functools.partial(dft_body, chunks, 1.0 / math.sqrt(lon_total)),
        grid_spec=pltpu.PrefetchScalarGridSpec(
            num_scalar_prefetch=1,
            grid=(groups,),
            in_specs=[
                whole(ocos.shape),
                whole(osin.shape),
                whole(icos.shape),
                whole(isin.shape),
                pl.BlockSpec((GROUP, row_count, lon_total), lambda g, *_: (g, 0, 0)),
                pl.BlockSpec(memory_space=pl.ANY),
            ],
            out_specs=[
                pl.BlockSpec(
                    (chunks, 1, GROUP + 1, 4 * SLOTS, LANES), lambda g, *_: (0, g, 0, 0, 0)
                )
                for _ in range(8)
            ],
            scratch_shapes=[
                pltpu.VMEM((lon_total, chunks * coefs), BF16),
                pltpu.VMEM((GROUP * row_count, coefs), BF16),
            ],
        ),
        out_shape=[out] * 8,
        compiler_params=pltpu.CompilerParams(
            dimension_semantics=("arbitrary",), vmem_limit_bytes=VMEM_LIMIT
        ),
        cost_estimate=pl.CostEstimate(
            flops=2 * chunks * coefs * field_count * row_count * lon_total,
            bytes_accessed=2 * grid_fields.size,
            transcendentals=0,
        ),
        name="dft",
    )(shift, ocos, osin, icos, isin, grid_fields, after)


def turn_body(leg_ref, after_ref, out_ref, tail):
    count, width, rows = leg_ref.shape
    even = rows - 1
    out_ref[: count * width, :] = leg_ref[:, :, :even].reshape(count * width, even)
    lane = lax.broadcasted_iota(jnp.int32, (16, LANES), 1)
    row = lax.broadcasted_iota(jnp.int32, (16, width), 0)
    first = jnp.where(lane == 0, 1.0, 0.0).astype(BF16)
    total = jnp.zeros((16, width), F32)
    for slot in range(count):
        column = jnp.broadcast_to(leg_ref[slot, :, even:].astype(F32), (width, LANES))
        total = jnp.where(row == slot, nt_dot(first, column.astype(BF16)), total)
    tail[...] = jnp.zeros_like(tail)
    tail[:, :width] = total
    out_ref[count * width :, :] = tail[...].astype(BF16)


def turn_call(at, legendre, after):
    width, rows = legendre.shape[1], legendre.shape[2]
    out = (SLOTS * width + 16, rows - 1)
    return pl.pallas_call(
        turn_body,
        grid=(1,),
        in_specs=[
            pl.BlockSpec((SLOTS, width, rows), lambda s: (at, 0, 0)),
            pl.BlockSpec(memory_space=pl.ANY),
        ],
        out_specs=pl.BlockSpec(out, lambda s: (0, 0)),
        out_shape=jax.ShapeDtypeStruct(out, BF16),
        scratch_shapes=[pltpu.VMEM((16, rows - 1), F32)],
        compiler_params=pltpu.CompilerParams(
            dimension_semantics=("arbitrary",), vmem_limit_bytes=VMEM_LIMIT
        ),
        cost_estimate=pl.CostEstimate(
            flops=2 * SLOTS * rows * width * width,
            bytes_accessed=4 * SLOTS * rows * width,
            transcendentals=0,
        ),
        name="turn",
    )(legendre, after)


def fold(arrived, sym, anti):
    small = LANES // GROUP
    halves = 4
    groups = arrived.shape[1]
    coefs = arrived.shape[3]
    rows = lax.broadcasted_iota(jnp.int32, (LANES, LANES), 0)
    columns = lax.broadcasted_iota(jnp.int32, (LANES, LANES), 1)
    mirror = picks(rows, LANES - 1 - columns)
    for lat in range(halves):
        north = arrived[lat, :, :GROUP].reshape(groups * GROUP * coefs, LANES).astype(F32)
        south = nn_dot(
            arrived[2 * halves - 1 - lat, :, :GROUP].reshape(groups * GROUP * coefs, LANES), mirror
        )
        sym[lat] = (north + south).astype(BF16).astype(F32)
        anti[lat] = (north - south).astype(BF16).astype(F32)
    wide = halves * LANES
    rows = lax.broadcasted_iota(jnp.int32, (wide, wide), 0)
    columns = lax.broadcasted_iota(jnp.int32, (wide, wide), 1)
    field, inside = columns // LANES, columns % LANES
    lat, place = inside // small, inside % small
    base = lat * LANES + field * small
    north = nn_dot(
        jnp.concatenate(
            [arrived[at, :, GROUP].reshape(groups * coefs, LANES) for at in range(halves)], axis=1
        ),
        picks(rows, base + place),
    )
    south = nn_dot(
        jnp.concatenate(
            [
                arrived[2 * halves - 1 - at, :, GROUP].reshape(groups * coefs, LANES)
                for at in range(halves)
            ],
            axis=1,
        ),
        picks(rows, base + small - 1 - place),
    )
    both = (north + south).astype(BF16).astype(F32), (north - south).astype(BF16).astype(F32)
    for group in range(groups):
        for at in range(GROUP):
            start = (group * GROUP + at) * coefs
            for ref, values in zip((sym, anti), both):
                ref[halves, start : start + coefs, :] = values[
                    group * coefs : (group + 1) * coefs, at * LANES : (at + 1) * LANES
                ]


def level_body(
    at, dims, pairs_ref, limits_ref, *refs
):
    field_count, wave_total, halves, fresh, piece = dims
    parts, rest = refs[:8], refs[8:]
    legendre, extra, one, two, three = rest[:5]
    rest = rest[6:] if fresh else rest[7:]
    spec_ref, outs, rest = rest[0], rest[1:9], rest[9:]
    arrived, send_ref, sems, sym, anti, gathered, main_n, main_s, small_n, small_s = rest
    slot = pl.program_id(0)
    lat = limits_ref[3]
    pair = pairs_ref[at * SLOTS + slot]
    stride = 4 * SLOTS
    both = 2 * field_count

    @pl.when(slot == 0)
    def _():
        copies = [
            pltpu.make_async_copy(parts[k].at[piece], arrived.at[jnp.bitwise_xor(lat, k)], sems.at[k])
            for k in range(8)
        ]
        for copy in copies:
            copy.start()
        for copy in copies:
            copy.wait()
        fold(arrived, sym, anti)
        for ref in (main_n, main_s, small_n, small_s):
            ref[...] = jnp.zeros_like(ref)

    def rows_of(ref):
        return jnp.concatenate(
            [
                jnp.concatenate(
                    [
                        ref[tile, pl.ds(c * 2 * SLOTS + 2 * slot + w, field_count, stride=stride), :]
                        for w in range(2)
                        for c in range(2)
                    ],
                    axis=0,
                )
                for tile in range(ref.shape[0])
            ],
            axis=1,
        )

    sym_rows, anti_rows = rows_of(sym), rows_of(anti)
    width = legendre.shape[1]
    table = jnp.concatenate(
        [legendre[g, :LANES, :] for g in range(4)] + [legendre[g, LANES:, :] for g in range(4)],
        axis=0,
    )
    stacked = jnp.concatenate([sym_rows, anti_rows], axis=0).astype(BF16)
    product = nn_dot(stacked, table)
    row_at = lax.broadcasted_iota(jnp.int32, (16, 2 * LANES), 0)
    lane_at = lax.broadcasted_iota(jnp.int32, (1, LANES), 1)
    small = width - LANES
    vector = []
    last = jnp.zeros((1, LANES), F32)
    for g in range(4):
        line = jnp.sum(
            jnp.where(row_at == slot, extra[g, :, : 2 * LANES].astype(F32), 0.0),
            axis=0,
            keepdims=True,
        )
        vector.append(line[:, :LANES])
        moved = line[:, LANES:]
        if g:
            moved = pltpu.roll(moved, g * small, 1)
        last = jnp.where(lane_at // small == g, moved, last)
    vector = jnp.concatenate(vector + [last], axis=1)
    final = jnp.sum(anti_rows * vector, axis=1, keepdims=True)

    lanes = wave_total
    rank = lax.broadcasted_iota(jnp.int32, (both, lanes), 1)
    sym_count = wave_total // 2 + 1
    sym_limit = (wave_total + 1 - pair) // 2
    anti_limit = (wave_total - pair) // 2
    spectrum = jnp.where(
        rank < sym_count,
        jnp.where(rank < sym_limit, product[:both], product[both : 2 * both]),
        jnp.where(
            rank < sym_count + anti_limit, product[2 * both : 3 * both], product[3 * both :]
        ),
    )
    final = jnp.where(lanes - sym_count < anti_limit, final[:both], final[both:])
    for tile in range(lanes // LANES):
        gathered[tile, pl.ds(slot, both, stride=SLOTS), :] = spectrum[
            :, tile * LANES : (tile + 1) * LANES
        ]
    gathered[lanes // LANES, pl.ds(slot, both, stride=SLOTS), :] = jnp.broadcast_to(
        final, (both, LANES)
    )
    kept = spectrum.astype(BF16).astype(F32)

    start = pl.multiple_of(slot * both, 16)
    for level, (ref, offset) in enumerate(((one, 0), (two, 384), (three, 0))):
        count = ref.shape[1]
        half = count // 2
        limit = limits_ref[level]
        place = lax.broadcasted_iota(jnp.int32, (both, 512), 1)
        first = jnp.where((place < half) & (pair + 2 * place <= limit), kept[:, :512], 0.0)
        moved = pltpu.roll(kept[:, :512], 512 - (sym_count - half), 1)
        second = jnp.where(
            (place >= half) & (place < count) & (pair + 1 + 2 * (place - half) <= limit),
            moved,
            0.0,
        )
        halfway = nn_dot(
            jnp.concatenate([first, second], axis=0)[:, :count].astype(BF16), ref[0]
        )
        even, odd = halfway[:both], halfway[both:]
        if level < 2:
            main_n[pl.ds(start, both), offset : offset + count] = (even + odd).astype(BF16)
            main_s[pl.ds(start, both), offset : offset + count] = (even - odd).astype(BF16)
        else:
            small_n[pl.ds(start, both), :count] = even + odd
            small_s[pl.ds(start, both), :count] = even - odd

    @pl.when(slot == SLOTS - 1)
    def _():
        for c in range(2):
            for tile in range(gathered.shape[0]):
                size = LANES if tile < lanes // LANES else 1
                spec_ref[:, c, :, tile * LANES : tile * LANES + size] = (
                    gathered[tile, c * field_count * SLOTS : (c + 1) * field_count * SLOTS, :size]
                    .astype(BF16)
                    .reshape(field_count, SLOTS, size)
                )
        own = [2 * ref.shape[1] // 8 for ref in (one, two, three)]
        wide = halves * LANES
        for north, main, tiny in ((True, main_n, small_n), (False, main_s, small_s)):
            rows = lax.broadcasted_iota(jnp.int32, (main.shape[1], wide), 0)
            columns = lax.broadcasted_iota(jnp.int32, (main.shape[1], wide), 1)
            owner, place = columns // LANES, columns % LANES
            late = place - own[0]
            if north:
                first = owner * own[0] + place
                second = 384 + owner * own[1] + late
            else:
                first = owner * own[0] + own[0] - 1 - place
                second = 384 + owner * own[1] + own[1] - 1 - late
            source = jnp.where(place < own[0], first, jnp.where(late < own[1], second, -1))
            moved = nn_dot(main[...], picks(rows, source)).astype(BF16)
            rows = lax.broadcasted_iota(jnp.int32, (LANES, wide), 0)
            columns = lax.broadcasted_iota(jnp.int32, (LANES, wide), 1)
            owner, place = columns // LANES, columns % LANES
            block, inside = place // 64, place % 64
            bundle, place = 3 * block + inside // own[2], inside % own[2]
            bundle = jnp.where(inside < 3 * own[2], bundle, -1)
            if not north:
                place = own[2] - 1 - place
            source = owner * own[2] + place
            tiles = tiny[...].reshape(SLOTS, both // 8, 8, LANES)
            packed = jnp.zeros((SLOTS * 8, wide), F32)
            for g in range(both // 8):
                packed = packed + nn_dot(
                    tiles[:, g].reshape(SLOTS * 8, LANES).astype(BF16),
                    picks(rows, jnp.where(bundle == g, source, -1)),
                )
            packed = packed.astype(BF16)
            for owner in range(halves):
                to = owner if north else 2 * halves - 1 - owner
                lanes_at = slice(owner * LANES, (owner + 1) * LANES)
                send_ref[to, : SLOTS * both, :] = moved[:, lanes_at]
                send_ref[to, SLOTS * both :, :] = packed[:, lanes_at]
        for k in range(8):
            outs[k][...] = send_ref[jnp.bitwise_xor(lat, k)]


def level_call(at, piece, pairs, limits, arrived, table, synths, after, spectrum, field_count):
    wave_total = table.shape[2]
    width = (table.shape[1] - 16) // SLOTS
    both = 2 * field_count
    fresh = spectrum is None
    dims = (field_count, wave_total, 4, fresh, piece)
    pair_local = pairs.shape[0]
    spec_shape = (field_count, 2, pair_local, wave_total + 1)
    rows = SLOTS * (both + 8)
    operands = [pairs, limits, *arrived, table, table, *synths, after]
    in_specs = [pl.BlockSpec(memory_space=pl.ANY) for _ in range(8)]
    in_specs += [
        pl.BlockSpec((4, width, wave_total), lambda s, *_: (0, s, 0)),
        pl.BlockSpec((4, 16, wave_total), lambda s, *_: (0, SLOTS * width // 16, 0)),
    ]
    in_specs += [
        pl.BlockSpec((1,) + ref.shape[1:], lambda s, *_: (at * SLOTS + s, 0, 0)) for ref in synths
    ]
    in_specs.append(pl.BlockSpec(memory_space=pl.ANY))
    aliases = {}
    if not fresh:
        operands.append(spectrum)
        in_specs.append(pl.BlockSpec(memory_space=pl.ANY))
        aliases = {len(operands) - 1: 0}
    flops = 2 * SLOTS * 4 * both * wave_total * wave_total
    made = pl.pallas_call(
        functools.partial(level_body, at, dims),
        grid_spec=pltpu.PrefetchScalarGridSpec(
            num_scalar_prefetch=2,
            grid=(SLOTS,),
            in_specs=in_specs,
            out_specs=[
                pl.BlockSpec(
                    (field_count, 2, SLOTS, wave_total + 1), lambda s, *_: (0, 0, at, 0)
                ),
            ]
            + [pl.BlockSpec((rows, LANES), lambda s, *_: (0, 0)) for _ in range(8)],
            scratch_shapes=[
                pltpu.VMEM((8,) + arrived[0].shape[1:], BF16),
                pltpu.VMEM((8, rows, LANES), BF16),
                pltpu.SemaphoreType.DMA((8,)),
                pltpu.VMEM((5, field_count * 4 * SLOTS, LANES), F32),
                pltpu.VMEM((5, field_count * 4 * SLOTS, LANES), F32),
                pltpu.VMEM((wave_total // LANES + 1, both * SLOTS, LANES), F32),
                pltpu.VMEM((SLOTS * both, 640), BF16),
                pltpu.VMEM((SLOTS * both, 640), BF16),
                pltpu.VMEM((SLOTS * both, LANES), F32),
                pltpu.VMEM((SLOTS * both, LANES), F32),
            ],
        ),
        out_shape=[jax.ShapeDtypeStruct(spec_shape, BF16)]
        + [jax.ShapeDtypeStruct((rows, LANES), BF16)] * 8,
        input_output_aliases=aliases,
        compiler_params=pltpu.CompilerParams(
            dimension_semantics=("arbitrary",), vmem_limit_bytes=VMEM_LIMIT
        ),
        cost_estimate=pl.CostEstimate(
            flops=flops, bytes_accessed=2 * table.size, transcendentals=0
        ),
        name="levels",
    )(*operands)
    return made[0], made[1:]


def inverse_body(chunks, field_step, lat_ref, *refs):
    arrived = refs[: chunks * 8]
    inv_one, inv_two, inv_three, out_one, out_two, out_three, main, tiny = refs[chunks * 8 :]
    lat = lat_ref[3]
    step = pl.program_id(0)
    both = 2 * out_three.shape[1]
    big = SLOTS * both
    small = SLOTS * 8

    @pl.when(step == 0)
    def _():
        for at in range(chunks):
            for k in range(8):
                place = at * 8 + jnp.bitwise_xor(lat, k)
                part = arrived[at * 8 + k]
                main[pl.ds(pl.multiple_of(place * big, 16), big), :] = part[:big, :].astype(F32)
                tiny[pl.ds(pl.multiple_of(place * small, 16), small), :] = part[big:, :].astype(F32)

    pairs = chunks * 8 * SLOTS
    own = out_one.shape[1]
    turned = []
    for at in range(field_step):
        field = step * field_step + at
        rows = jnp.concatenate(
            [main[pl.ds(c * (both // 2) + field, pairs, stride=both), :] for c in range(2)], axis=0
        )
        turned.append(rows.T.astype(BF16))
    grid_rows = nn_dot(jnp.concatenate([x[:own] for x in turned], axis=0), inv_one[...])
    for at in range(field_step):
        out_one[at] = grid_rows[at * own : (at + 1) * own]
    rest = LANES - own
    grid_rows = nn_dot(jnp.concatenate([x[own:] for x in turned], axis=0), inv_two[...])
    for at in range(field_step):
        out_two[at] = grid_rows[at * rest : at * rest + out_two.shape[1]]

    @pl.when(step < 4)
    def _():
        for at in range(2):
            inside = 2 * step + at
            rows = tiny[pl.ds(inside, pairs, stride=8), :]
            turned = rows.T.astype(BF16)
            grid_rows = nn_dot(turned[:64], inv_three[:pairs]) + nn_dot(
                turned[64:], inv_three[pairs:]
            )
            count = out_three.shape[0]
            for bundle in range(3):
                for row in range(count):
                    out_three[row, pl.ds(bundle * 8 + inside, 1), :] = grid_rows[
                        bundle * count + row : bundle * count + row + 1
                    ]


def inverse_call(limits, arrived, tables, field_count):
    chunks = len(arrived)
    field_step = 4
    both = 2 * field_count
    whole = lambda shape: pl.BlockSpec(shape, lambda g, *_: (0,) * len(shape))
    flat = [x for parts in arrived for x in parts]
    outs = [(field_count, t.shape[1] // 16, t.shape[1]) for t in tables]
    outs[2] = (outs[2][1], outs[2][0], outs[2][2])
    one, two, three = pl.pallas_call(
        functools.partial(inverse_body, chunks, field_step),
        grid_spec=pltpu.PrefetchScalarGridSpec(
            num_scalar_prefetch=1,
            grid=(field_count // field_step,),
            in_specs=[whole(x.shape) for x in flat] + [whole(t.shape) for t in tables],
            out_specs=[
                pl.BlockSpec((field_step,) + outs[0][1:], lambda g, *_: (g, 0, 0)),
                pl.BlockSpec((field_step,) + outs[1][1:], lambda g, *_: (g, 0, 0)),
                whole(outs[2]),
            ],
            scratch_shapes=[
                pltpu.VMEM((chunks * 8 * SLOTS * both, LANES), F32),
                pltpu.VMEM((chunks * 8 * SLOTS * 8, LANES), F32),
            ],
        ),
        out_shape=[jax.ShapeDtypeStruct(shape, F32) for shape in outs],
        compiler_params=pltpu.CompilerParams(
            dimension_semantics=("arbitrary",), vmem_limit_bytes=VMEM_LIMIT
        ),
        cost_estimate=pl.CostEstimate(
            flops=2 * field_count * LANES * both * 640, bytes_accessed=1 << 24, transcendentals=0
        ),
        name="inverse",
    )(limits, *flat, *tables)
    return one, two, three.transpose(1, 0, 2)


def wave_trig(waves, length):
    step = 2.0 * math.pi / length

    def angles(places):
        return ((places[:, None] * waves[None, :]) % length).astype(F32) * step

    outer = angles(jnp.arange(length // LANES, dtype=jnp.int32) * LANES)
    inner = angles(jnp.arange(LANES, dtype=jnp.int32))
    return jnp.cos(outer), jnp.sin(outer), jnp.cos(inner), jnp.sin(inner)


def chunked_on_device(grid_fields, assign, limits, legendre, synth_one, synth_two, synth_three):
    lat_count = lax.axis_size("lat")
    field_count, row_count, lon_total = grid_fields.shape
    pair_total = assign.shape[0]
    pair_local = pair_total // lat_count
    wave_total = 2 * pair_total
    chunks = pair_local // SLOTS
    synths = (synth_one, synth_two, synth_three)
    lat = lax.axis_index("lat")
    by_owner = assign.reshape(lat_count, chunks, SLOTS)
    own_pairs = lax.dynamic_slice(assign, (lat * pair_local,), (pair_local,))
    south = (lat >= lat_count // 2).astype(jnp.int32)
    small = row_count - LANES
    shift = jnp.stack([south * small, (1 - south) * LANES])

    scalars = jnp.concatenate([limits, lat.astype(jnp.int32)[None]])
    partners = jnp.bitwise_xor(lat, jnp.arange(lat_count, dtype=jnp.int32))
    to_partner = jnp.take(by_owner, partners, axis=0)
    turned = legendre.transpose(0, 2, 1)
    waves = jnp.stack([to_partner, wave_total - 1 - to_partner], axis=3)
    waves = waves.transpose(1, 0, 2, 3).reshape(chunks, -1)

    def exchange(parts):
        return [parts[0]] + [
            lax.ppermute(parts[k], "lat", [(i, i ^ k) for i in range(lat_count)])
            for k in range(1, lat_count)
        ]

    def gather(at, after):
        packed = turn_call(at, turned, after)
        return packed, lax.all_gather(packed, "fld")

    spans = [(0, 1)] + [(at, min(at + 2, chunks)) for at in range(1, chunks, 2)]
    packed, table = gather(0, assign)
    tables = [table]
    crossed = []
    after = packed
    for first, last in spans:
        trig = wave_trig(waves[first:last].reshape(-1), lon_total)
        sent = dft_call(shift, trig, grid_fields, after)
        after = sent[0]
        moved = exchange(sent)
        crossed += [(moved, piece) for piece in range(last - first)]
        tables += [gather(chunk, after)[1] for chunk in range(max(first, 1), last)]

    order = by_owner.transpose(1, 0, 2).reshape(-1)
    inverses = [both_parts(order, 4 * table.shape[1]) for table in synths]
    spectrum = None
    arrived = []
    for at in range(chunks):
        after = inverses[at % 3]
        moved, piece = crossed[at]
        spectrum, send = level_call(
            at, piece, own_pairs, scalars, moved, tables[at], synths, after, spectrum, field_count
        )
        arrived.append(exchange(send))
    return (spectrum, *inverse_call(scalars, arrived, inverses, field_count))


def both_parts(order, length):
    weight = jnp.where(order == 0, 1.0, 2.0).astype(F32) / math.sqrt(length)
    waves = jnp.concatenate([order, order])
    quarters = jnp.concatenate([jnp.zeros_like(order), jnp.ones_like(order)])
    table = turned_cosine(waves, quarters, jnp.arange(length, dtype=jnp.int32))
    return (table * jnp.concatenate([weight, weight])[:, None]).astype(BF16)


def on_device(*arguments):
    if fits(*arguments):
        return chunked_on_device(*arguments)
    return plain_on_device(*arguments)


def solution(mesh):
    return jax.shard_map(
        on_device,
        mesh=mesh,
        in_specs=(
            P("fld", "lat", None),
            P(),
            P(),
            P("lat", None, "fld"),
            P("lat", None, None),
            P("lat", None, None),
            P("lat", None, None),
        ),
        out_specs=(
            P("fld", None, "lat", None),
            P("fld", "lat", None),
            P("fld", "lat", None),
            P("fld", "lat", None),
        ),
        check_vma=False,
    )
```

```python
import functools
import math

import jax
import jax.numpy as jnp
from jax import lax
from jax.experimental import pallas as pl
from jax.experimental.pallas import tpu as pltpu
from jax.sharding import PartitionSpec as P


CHUNKS = 1


def choose_pair(values, limit_of):
    ranks = jnp.arange(values.shape[-1], dtype=jnp.int32)
    keep_mask = ranks[None, :] < limit_of[:, None]
    return jnp.where(keep_mask[None, None], values[:, :, :, 0], values[:, :, :, 1])


def select_rows(sym_prod, anti_prod, own_pairs, wave_total):
    first_rows = choose_pair(sym_prod, (wave_total + 1 - own_pairs) // 2)
    later_rows = choose_pair(anti_prod, (wave_total - own_pairs) // 2)
    return jnp.concatenate([first_rows, later_rows], axis=3)


def level_rows_of(spectrum, own_pairs, limit, synth_table, lat_count):
    half_rows = synth_table.shape[1] // 2
    sym_rows = spectrum.shape[3] // 2 + 1
    step_rows = 2 * jnp.arange(half_rows, dtype=jnp.int32)
    keep_sym = own_pairs[:, None] + step_rows[None, :] <= limit
    keep_anti = own_pairs[:, None] + 1 + step_rows[None, :] <= limit
    zero_value = jnp.zeros((), jnp.bfloat16)
    kept_sym = jnp.where(keep_sym[None, None], spectrum[..., :half_rows], zero_value)
    kept_anti = jnp.where(
        keep_anti[None, None], spectrum[..., sym_rows : sym_rows + half_rows], zero_value
    )
    even_part = jnp.einsum(
        "fcqk,qkj->qcfj", kept_sym, synth_table[:, :half_rows], preferred_element_type=jnp.float32
    )
    odd_part = jnp.einsum(
        "fcqk,qkj->qcfj", kept_anti, synth_table[:, half_rows:], preferred_element_type=jnp.float32
    )
    north = (even_part + odd_part).astype(jnp.bfloat16)
    south = jnp.flip((even_part - odd_part).astype(jnp.bfloat16), axis=3)
    slots, parts, fields, half_lat = north.shape
    owners = lat_count // 2
    halves = [
        part.reshape(slots * parts, fields, owners, half_lat // owners)
        .transpose(2, 0, 1, 3)
        .reshape(owners, slots * parts, -1)
        for part in (north, south)
    ]
    return jnp.concatenate(halves, axis=0)


def quarter_of(values, axis):
    return lax.broadcasted_iota(jnp.int32, values.shape, axis).reshape(-1)


def turned_cosine(waves, quarters, places):
    length = places.shape[0]
    inner = 128 if length % 128 == 0 else math.gcd(length, 128)
    coarse = jnp.arange(length // inner, dtype=jnp.int32) * inner
    fine = jnp.arange(inner, dtype=jnp.int32)
    step = 2.0 * math.pi / length

    def angles(at, shift):
        return ((waves[:, None] * at[None, :] + shift) % length).astype(jnp.float32) * step

    outer_angle = angles(coarse, quarters[:, None] * (length // 4))
    inner_angle = angles(fine, 0)
    outer_cos, outer_sin = jnp.cos(outer_angle), jnp.sin(outer_angle)
    inner_cos, inner_sin = jnp.cos(inner_angle), jnp.sin(inner_angle)
    outer_cos, outer_sin, inner_cos, inner_sin = lax.optimization_barrier(
        (outer_cos, outer_sin, inner_cos, inner_sin)
    )
    pieces = [
        outer_cos[:, at : at + 1] * inner_cos - outer_sin[:, at : at + 1] * inner_sin
        for at in range(length // inner)
    ]
    return jnp.concatenate(pieces, axis=1)


def inverse_table(order, lon_length):
    waves = jnp.stack([order, order], axis=1)
    weight = jnp.where(waves == 0, 1.0, 2.0).astype(jnp.float32) / math.sqrt(lon_length)
    places = jnp.arange(lon_length, dtype=jnp.int32)
    table = turned_cosine(waves.reshape(-1), quarter_of(waves, 1), places)
    return (table * weight.reshape(-1)[:, None]).astype(jnp.bfloat16)


def plain_on_device(grid_fields, assign, limits, legendre, synth_one, synth_two, synth_three):
    lat_count = lax.axis_size("lat")
    field_count, row_count, lon_total = grid_fields.shape
    pair_total = assign.shape[0]
    pair_local = pair_total // lat_count
    wave_total = 2 * pair_total
    sym_rows = pair_total + 1
    chunks = CHUNKS
    while pair_local % chunks:
        chunks -= 1
    slots = pair_local // chunks
    half_count = lat_count // 2
    synth_tables = (synth_one, synth_two, synth_three)
    dft_scale = 1.0 / math.sqrt(lon_total)
    flat_grid = grid_fields.reshape(field_count * row_count, lon_total)
    by_owner = assign.reshape(lat_count, chunks, slots)
    own_all = lax.dynamic_index_in_dim(by_owner, lax.axis_index("lat"), 0, keepdims=False)

    places = jnp.arange(lon_total, dtype=jnp.int32)
    sent_rows = []
    gathered = []
    for at in range(chunks):
        own_block = legendre[at * slots : (at + 1) * slots]
        gathered.append(
            [
                lax.all_gather(part, "fld", axis=2, tiled=True)
                for part in (own_block[:, :sym_rows], own_block[:, sym_rows:])
            ]
        )
    for at in range(chunks):
        waves = jnp.stack([by_owner[:, at], wave_total - 1 - by_owner[:, at]], axis=2)
        waves = jnp.stack([waves, waves], axis=1)
        dft_table = (
            turned_cosine(waves.reshape(-1), quarter_of(waves, 1), places) * dft_scale
        ).astype(jnp.bfloat16)
        fourier = lax.dot_general(
            dft_table,
            flat_grid,
            (((1,), (1,)), ((), ())),
            preferred_element_type=jnp.float32,
        ).astype(jnp.bfloat16)
        sent_rows.append(
            lax.all_to_all(
                fourier.reshape(lat_count, 4 * slots, field_count * row_count),
                "lat",
                split_axis=0,
                concat_axis=0,
                tiled=True,
            )
        )

    spectra = []
    arrived = []
    for at in range(chunks):
        own_pairs = own_all[at]
        split_six = (
            sent_rows[at]
            .reshape(lat_count, 2, slots, 2, field_count, row_count)
            .transpose(2, 1, 3, 4, 0, 5)
        )
        flat_shape = (slots, 2, 2, field_count, half_count * row_count)
        split_six = lax.optimization_barrier(split_six)
        north_rows = split_six[..., :half_count, :].reshape(flat_shape).astype(jnp.float32)
        south_rows = jnp.flip(split_six[..., half_count:, :].reshape(flat_shape), axis=4).astype(
            jnp.float32
        )
        symmetric = (north_rows + south_rows).astype(jnp.bfloat16)
        antisym = (north_rows - south_rows).astype(jnp.bfloat16)
        block_piece = gathered[at]
        sym_add = jnp.einsum(
            "scwkj,srj->kcswr",
            symmetric,
            block_piece[0],
            preferred_element_type=jnp.float32,
        )
        anti_add = jnp.einsum(
            "scwkj,srj->kcswr",
            antisym,
            block_piece[1],
            preferred_element_type=jnp.float32,
        )
        spectrum = select_rows(sym_add, anti_add, own_pairs, wave_total).astype(jnp.bfloat16)
        spectra.append(spectrum)
        level_blocks = [
            level_rows_of(
                spectrum,
                own_pairs,
                limits[level],
                synth_tables[level][at * slots : (at + 1) * slots],
                lat_count,
            )
            for level in range(3)
        ]
        arrived.append(
            lax.all_to_all(
                jnp.concatenate(level_blocks, axis=2),
                "lat",
                split_axis=0,
                concat_axis=0,
                tiled=True,
            )
        )

    order = by_owner.transpose(1, 0, 2).reshape(-1)
    all_rows = jnp.stack(arrived, axis=0).reshape(2 * pair_total, -1)
    grids_out = []
    start = 0
    for level in range(3):
        level_lat = 2 * synth_tables[level].shape[1]
        own_rows = level_lat // lat_count
        width = field_count * own_rows
        inverse = inverse_table(order, 2 * level_lat)
        grids_out.append(
            lax.dot_general(
                all_rows[:, start : start + width],
                inverse,
                (((0,), (0,)), ((), ())),
                preferred_element_type=jnp.float32,
            ).reshape(field_count, own_rows, -1)
        )
        start += width
    return (jnp.concatenate(spectra, axis=2), grids_out[0], grids_out[1], grids_out[2])


F32 = jnp.float32
BF16 = jnp.bfloat16
LANES = 128
GROUP = 4
SLOTS = 8
PITCH = 40
SPREAD = 56
VMEM_LIMIT = 56 * 1024 * 1024


def fits(grid_fields, assign, limits, legendre, synth_one, synth_two, synth_three):
    field_count, row_count, lon_total = grid_fields.shape
    lat_count = lax.axis_size("lat")
    pair_local = assign.shape[0] // lat_count
    rest = row_count - LANES
    counts = (synth_one.shape[1], synth_two.shape[1], synth_three.shape[1])
    owns = [2 * count // lat_count for count in counts]
    return (
        lat_count == 8
        and lax.axis_size("fld") * row_count == legendre.shape[2] * lax.axis_size("fld")
        and lax.axis_size("fld") == lat_count // 2
        and rest * GROUP == LANES
        and field_count == 6 * GROUP
        and lon_total % LANES == 0
        and pair_local % SLOTS == 0
        and legendre.shape[1] == 2 * assign.shape[0] + 1
        and (2 * assign.shape[0]) % LANES == 0
        and owns[0] % 16 == 0
        and owns[0] + owns[1] + 8 == LANES
        and 3 * owns[2] <= 64
        and counts[0] <= 384
        and counts[1] <= 256
        and counts[2] <= LANES
    )


def nt_dot(left, right):
    return lax.dot_general(left, right, (((1,), (1,)), ((), ())), preferred_element_type=F32)


def nn_dot(left, right):
    return jnp.dot(left, right, preferred_element_type=F32)


def picks(rows, source):
    return jnp.where(rows == source, 1.0, 0.0).astype(BF16)


def turn_cosine(product, length):
    turns = jnp.floor(product * (1.0 / length))
    place = product - turns * length
    angle = (length / 4 - jnp.abs(place - length / 2)) * (2.0 * math.pi / length)
    square = angle * angle
    value = jnp.full_like(angle, 1.0 / math.factorial(13))
    for order in (11, 9, 7, 5, 3, 1):
        sign = 1.0 if order % 4 == 1 else -1.0
        value = value * square + sign / math.factorial(order)
    return -(value * angle)


def dft_body(groups, length, shift_ref, waves_ref, grid_ref, after_ref, *rest):
    chunks = sum(groups)
    count = 8 * len(groups)
    outs, table, stage = rest[:count], rest[count], rest[count + 1]
    per_slot = 2 * SLOTS
    side = 8 * per_slot
    coefs = 2 * side
    steps = length // LANES
    scale = 1.0 / math.sqrt(length)

    @pl.when(pl.program_id(0) == 0)
    def _():
        inner_at = lax.broadcasted_iota(jnp.int32, (LANES, side), 0).astype(F32)
        outer_at = lax.broadcasted_iota(jnp.int32, (8 * pl.cdiv(steps, 8), side), 0).astype(F32)
        for at in range(chunks):
            waves = waves_ref[:, at * side : (at + 1) * side]
            inner = inner_at * waves
            outer = outer_at * (waves * LANES)
            cos_in = turn_cosine(inner, length) * scale
            sin_in = turn_cosine(inner + 0.75 * length, length) * scale
            cos_all = turn_cosine(outer, length)
            sin_all = turn_cosine(outer + 0.75 * length, length)
            for step in range(steps):
                cos_out, sin_out = cos_all[step : step + 1], sin_all[step : step + 1]
                rows = slice(step * LANES, (step + 1) * LANES)
                table[rows, at * coefs : at * coefs + side] = (
                    cos_out * cos_in - sin_out * sin_in
                ).astype(BF16)
                table[rows, at * coefs + side : (at + 1) * coefs] = (
                    -(sin_out * cos_in + cos_out * sin_in)
                ).astype(BF16)

    group, row_count, lon_total = grid_ref.shape
    small = row_count - LANES
    first = pl.multiple_of(shift_ref[0], 16)
    second = pl.multiple_of(shift_ref[1], 16)
    stage[...] = nn_dot(grid_ref[...].reshape(group * row_count, lon_total), table[...]).astype(BF16)
    at = 0
    for place, size in enumerate(groups):
        for piece in range(size):
            lanes = slice(at * coefs, (at + 1) * coefs)
            pieces = [stage[pl.ds(f * row_count + first, LANES), lanes] for f in range(group)]
            pieces += [stage[pl.ds(f * row_count + second, small), lanes] for f in range(group)]
            turned = jnp.concatenate(pieces, axis=0).T
            for k in range(8):
                for c in range(2):
                    start = c * side + k * per_slot
                    for tile in range(group + 1):
                        outs[place * 8 + k][piece, 0, tile, c * per_slot : (c + 1) * per_slot, :] = (
                            turned[start : start + per_slot, tile * LANES : (tile + 1) * LANES]
                        )
            at += 1


def dft_call(groups, shift, waves, grid_fields, after):
    field_count, row_count, lon_total = grid_fields.shape
    chunks = sum(groups)
    coefs = 8 * 4 * SLOTS
    steps = field_count // GROUP
    tail = (GROUP + 1, 4 * SLOTS, LANES)
    sizes = [size for size in groups for _ in range(8)]
    sent = pl.pallas_call(
        functools.partial(dft_body, groups, lon_total),
        grid_spec=pltpu.PrefetchScalarGridSpec(
            num_scalar_prefetch=1,
            grid=(steps,),
            in_specs=[
                pl.BlockSpec(waves.shape, lambda g, *_: (0, 0)),
                pl.BlockSpec((GROUP, row_count, lon_total), lambda g, *_: (g, 0, 0)),
                pl.BlockSpec(memory_space=pl.ANY),
            ],
            out_specs=[
                pl.BlockSpec((size, 1) + tail, lambda g, *_: (0, g, 0, 0, 0)) for size in sizes
            ],
            scratch_shapes=[
                pltpu.VMEM((lon_total, chunks * coefs), BF16),
                pltpu.VMEM((GROUP * row_count, chunks * coefs), BF16),
            ],
        ),
        out_shape=[jax.ShapeDtypeStruct((size, steps) + tail, BF16) for size in sizes],
        compiler_params=pltpu.CompilerParams(
            dimension_semantics=("arbitrary",), vmem_limit_bytes=VMEM_LIMIT
        ),
        cost_estimate=pl.CostEstimate(
            flops=2 * chunks * coefs * field_count * row_count * lon_total,
            bytes_accessed=2 * grid_fields.size,
            transcendentals=0,
        ),
        name="dft",
    )(shift, waves, grid_fields, after)
    return [sent[at * 8 : (at + 1) * 8] for at in range(len(groups))]


def tables_body(waves_ref, after_ref, *outs):
    waves = waves_ref[...]
    block = waves.shape[0]
    part = pl.program_id(0) // (pl.num_programs(0) // 2)
    for out in outs:
        length = 2 * (out.shape[1] // 2)
        weight = jnp.where(waves == 0.0, 1.0, 2.0) / math.sqrt(length)
        for start in range(0, length, LANES):
            size = min(LANES, length - start)
            places = lax.broadcasted_iota(jnp.int32, (block, size), 1) + start
            product = waves * places.astype(F32) + jnp.where(part == 0, 0.0, 0.25 * length)
            out[:, start : start + size] = (turn_cosine(product, length) * weight).astype(BF16)


def tables_call(order, lengths, after):
    count = order.shape[0]
    block = 64
    steps = count // block
    waves = order.astype(F32)[:, None]
    return pl.pallas_call(
        tables_body,
        grid=(2 * steps,),
        in_specs=[
            pl.BlockSpec((block, 1), lambda g: (g % steps, 0)),
            pl.BlockSpec(memory_space=pl.ANY),
        ],
        out_specs=[pl.BlockSpec((block, length), lambda g: (g, 0)) for length in lengths],
        out_shape=[jax.ShapeDtypeStruct((2 * count, length), BF16) for length in lengths],
        compiler_params=pltpu.CompilerParams(
            dimension_semantics=("arbitrary",), vmem_limit_bytes=VMEM_LIMIT
        ),
        cost_estimate=pl.CostEstimate(flops=10**9, bytes_accessed=10**7, transcendentals=0),
        name="tables",
    )(waves, after)


def turn_body(leg_ref, after_ref, out_ref, tail):
    count, width, rows = leg_ref.shape
    even = rows - 1
    out_ref[0, : count * width, :] = leg_ref[:, :, :even].reshape(count * width, even)
    lane = lax.broadcasted_iota(jnp.int32, (16, LANES), 1)
    row = lax.broadcasted_iota(jnp.int32, (16, width), 0)
    first = jnp.where(lane == 0, 1.0, 0.0).astype(BF16)
    total = jnp.zeros((16, width), F32)
    for slot in range(count):
        column = jnp.broadcast_to(leg_ref[slot, :, even:].astype(F32), (width, LANES))
        total = jnp.where(row == slot, nt_dot(first, column.astype(BF16)), total)
    tail[...] = jnp.zeros_like(tail)
    tail[:, :width] = total
    out_ref[0, count * width :, :] = tail[...].astype(BF16)


def turn_call(first, last, legendre, after):
    width, rows = legendre.shape[1], legendre.shape[2]
    out = (SLOTS * width + 16, rows - 1)
    count = last - first
    return pl.pallas_call(
        turn_body,
        grid=(count,),
        in_specs=[
            pl.BlockSpec((SLOTS, width, rows), lambda s: (first + s, 0, 0)),
            pl.BlockSpec(memory_space=pl.ANY),
        ],
        out_specs=pl.BlockSpec((1,) + out, lambda s: (s, 0, 0)),
        out_shape=jax.ShapeDtypeStruct((count,) + out, BF16),
        scratch_shapes=[pltpu.VMEM((16, rows - 1), F32)],
        compiler_params=pltpu.CompilerParams(
            dimension_semantics=("arbitrary",), vmem_limit_bytes=VMEM_LIMIT
        ),
        cost_estimate=pl.CostEstimate(
            flops=2 * count * SLOTS * rows * width * width,
            bytes_accessed=4 * count * SLOTS * rows * width,
            transcendentals=0,
        ),
        name="turn",
    )(legendre, after)


def fold(arrived, sym, anti, here):
    small = LANES // GROUP
    halves = 4
    groups = arrived.shape[1]
    coefs = arrived.shape[3]
    rows = lax.broadcasted_iota(jnp.int32, (LANES, LANES), 0)
    columns = lax.broadcasted_iota(jnp.int32, (LANES, LANES), 1)
    mirror = picks(rows, LANES - 1 - columns)
    for lat in range(halves):
        north = arrived[lat, :, :GROUP].reshape(groups * GROUP * coefs, LANES).astype(F32)
        south = nn_dot(
            arrived[2 * halves - 1 - lat, :, :GROUP].reshape(groups * GROUP * coefs, LANES), mirror
        )
        for ref, values in ((sym, north + south), (anti, north - south)):
            values = values.astype(BF16).astype(F32)
            for field in range(groups * GROUP):
                ref[lat, field * PITCH : field * PITCH + coefs, :] = values[
                    field * coefs : (field + 1) * coefs
                ]
    wide = halves * LANES
    rows = lax.broadcasted_iota(jnp.int32, (wide, wide), 0)
    columns = lax.broadcasted_iota(jnp.int32, (wide, wide), 1)
    field, inside = columns // LANES, columns % LANES
    lat, place = jnp.bitwise_xor(inside // small, here), inside % small
    base = lat * LANES + field * small
    north = nn_dot(
        jnp.concatenate(
            [arrived[at, :, GROUP].reshape(groups * coefs, LANES) for at in range(halves)], axis=1
        ),
        picks(rows, base + place),
    )
    south = nn_dot(
        jnp.concatenate(
            [
                arrived[2 * halves - 1 - at, :, GROUP].reshape(groups * coefs, LANES)
                for at in range(halves)
            ],
            axis=1,
        ),
        picks(rows, base + small - 1 - place),
    )
    both = (north + south).astype(BF16).astype(F32), (north - south).astype(BF16).astype(F32)
    for group in range(groups):
        for at in range(GROUP):
            start = (group * GROUP + at) * PITCH
            for ref, values in zip((sym, anti), both):
                ref[halves, start : start + coefs, :] = values[
                    group * coefs : (group + 1) * coefs, at * LANES : (at + 1) * LANES
                ]


def level_body(
    at, dims, pairs_ref, limits_ref, *refs
):
    field_count, wave_total, halves, fresh, piece = dims
    parts, legendre, extra, rest = refs[:8], refs[8:12], refs[12:16], refs[16:]
    one, two, three = rest[:3]
    rest = rest[4:] if fresh else rest[5:]
    spec_ref, outs, rest = rest[0], rest[1:9], rest[9:]
    arrived, send_ref, sems, sym, anti, gathered, main_n, main_s, small_n, small_s = rest
    slot = pl.program_id(0)
    lat, here = limits_ref[3], limits_ref[4]
    pair = pairs_ref[at * SLOTS + slot]
    stride = PITCH
    both = 2 * field_count

    @pl.when(slot == 0)
    def _():
        copies = [
            pltpu.make_async_copy(parts[k].at[piece], arrived.at[jnp.bitwise_xor(lat, k)], sems.at[k])
            for k in range(8)
        ]
        for copy in copies:
            copy.start()
        for copy in copies:
            copy.wait()
        fold(arrived, sym, anti, here)
        for ref in (main_n, main_s, small_n, small_s):
            ref[...] = jnp.zeros_like(ref)

    def rows_of(ref):
        return jnp.concatenate(
            [
                jnp.concatenate(
                    [
                        ref[
                            jnp.bitwise_xor(here, tile) if tile < 4 else tile,
                            pl.ds(c * 2 * SLOTS + 2 * slot + w, field_count, stride=stride),
                            :,
                        ]
                        for w in range(2)
                        for c in range(2)
                    ],
                    axis=0,
                )
                for tile in range(ref.shape[0])
            ],
            axis=1,
        )

    sym_rows, anti_rows = rows_of(sym), rows_of(anti)
    width = legendre[0].shape[1]
    table = jnp.concatenate(
        [ref[0, :LANES, :] for ref in legendre] + [ref[0, LANES:, :] for ref in legendre], axis=0
    )
    stacked = jnp.concatenate([sym_rows, anti_rows], axis=0).astype(BF16)
    product = nn_dot(stacked, table)
    row_at = lax.broadcasted_iota(jnp.int32, (16, 2 * LANES), 0)
    lane_at = lax.broadcasted_iota(jnp.int32, (1, LANES), 1)
    small = width - LANES
    vector = []
    last = jnp.zeros((1, LANES), F32)
    for g in range(4):
        line = jnp.sum(
            jnp.where(row_at == slot, extra[g][0, :, : 2 * LANES].astype(F32), 0.0),
            axis=0,
            keepdims=True,
        )
        vector.append(line[:, :LANES])
        moved = line[:, LANES:]
        if g:
            moved = pltpu.roll(moved, g * small, 1)
        last = jnp.where(lane_at // small == g, moved, last)
    vector = jnp.concatenate(vector + [last], axis=1)
    final = jnp.sum(anti_rows * vector, axis=1, keepdims=True)

    lanes = wave_total
    rank = lax.broadcasted_iota(jnp.int32, (both, lanes), 1)
    sym_count = wave_total // 2 + 1
    sym_limit = (wave_total + 1 - pair) // 2
    anti_limit = (wave_total - pair) // 2
    spectrum = jnp.where(
        rank < sym_count,
        jnp.where(rank < sym_limit, product[:both], product[both : 2 * both]),
        jnp.where(
            rank < sym_count + anti_limit, product[2 * both : 3 * both], product[3 * both :]
        ),
    )
    final = jnp.where(lanes - sym_count < anti_limit, final[:both], final[both:])
    for tile in range(lanes // LANES):
        gathered[tile, pl.ds(slot, both, stride=SLOTS), :] = spectrum[
            :, tile * LANES : (tile + 1) * LANES
        ]
    gathered[lanes // LANES, pl.ds(slot, both, stride=SLOTS), :] = jnp.broadcast_to(
        final, (both, LANES)
    )
    kept = spectrum.astype(BF16).astype(F32)

    start = pl.multiple_of(slot * both, 16)
    for level, (ref, offset) in enumerate(((one, 0), (two, 384), (three, 0))):
        count = ref.shape[1]
        half = count // 2
        limit = limits_ref[level]
        place = lax.broadcasted_iota(jnp.int32, (both, 512), 1)
        first = jnp.where((place < half) & (pair + 2 * place <= limit), kept[:, :512], 0.0)
        moved = pltpu.roll(kept[:, :512], 512 - (sym_count - half), 1)
        second = jnp.where(
            (place >= half) & (place < count) & (pair + 1 + 2 * (place - half) <= limit),
            moved,
            0.0,
        )
        halfway = nn_dot(
            jnp.concatenate([first, second], axis=0)[:, :count].astype(BF16), ref[0]
        )
        even, odd = halfway[:both], halfway[both:]
        if level < 2:
            main_n[pl.ds(start, both), offset : offset + count] = (even + odd).astype(BF16)
            main_s[pl.ds(start, both), offset : offset + count] = (even - odd).astype(BF16)
        else:
            small_n[pl.ds(start, both), :count] = even + odd
            small_s[pl.ds(start, both), :count] = even - odd

    @pl.when(slot == SLOTS - 1)
    def _():
        for c in range(2):
            for tile in range(gathered.shape[0]):
                size = LANES if tile < lanes // LANES else 1
                spec_ref[:, c, :, tile * LANES : tile * LANES + size] = (
                    gathered[tile, c * field_count * SLOTS : (c + 1) * field_count * SLOTS, :size]
                    .astype(BF16)
                    .reshape(field_count, SLOTS, size)
                )
        own = [2 * ref.shape[1] // 8 for ref in (one, two, three)]
        wide = halves * LANES
        for north, main, tiny in ((True, main_n, small_n), (False, main_s, small_s)):
            rows = lax.broadcasted_iota(jnp.int32, (main.shape[1], wide), 0)
            columns = lax.broadcasted_iota(jnp.int32, (main.shape[1], wide), 1)
            owner, place = columns // LANES, columns % LANES
            late = place - own[0]
            if north:
                first = owner * own[0] + place
                second = 384 + owner * own[1] + late
            else:
                first = owner * own[0] + own[0] - 1 - place
                second = 384 + owner * own[1] + own[1] - 1 - late
            source = jnp.where(place < own[0], first, jnp.where(late < own[1], second, -1))
            moved = nn_dot(main[...], picks(rows, source)).astype(BF16)
            rows = lax.broadcasted_iota(jnp.int32, (LANES, wide), 0)
            columns = lax.broadcasted_iota(jnp.int32, (LANES, wide), 1)
            owner, place = columns // LANES, columns % LANES
            block, inside = place // 64, place % 64
            bundle, place = 3 * block + inside // own[2], inside % own[2]
            bundle = jnp.where(inside < 3 * own[2], bundle, -1)
            if not north:
                place = own[2] - 1 - place
            source = owner * own[2] + place
            tiles = tiny[...].reshape(SLOTS, both // 8, 8, LANES)
            packed = jnp.zeros((SLOTS * 8, wide), F32)
            for g in range(both // 8):
                packed = packed + nn_dot(
                    tiles[:, g].reshape(SLOTS * 8, LANES).astype(BF16),
                    picks(rows, jnp.where(bundle == g, source, -1)),
                )
            packed = packed.astype(BF16)
            for owner in range(halves):
                to = owner if north else 2 * halves - 1 - owner
                lanes_at = slice(owner * LANES, (owner + 1) * LANES)
                send_ref[to, : SLOTS * both, :] = moved[:, lanes_at]
                send_ref[to, SLOTS * both :, :] = packed[:, lanes_at]
        for k in range(8):
            outs[k][...] = send_ref[jnp.bitwise_xor(lat, k)]


def level_call(at, piece, own, pairs, limits, arrived, table, synths, after, spectrum, field_count):
    wave_total = table[0].shape[2]
    width = (table[0].shape[1] - 16) // SLOTS
    both = 2 * field_count
    fresh = spectrum is None
    dims = (field_count, wave_total, 4, fresh, piece)
    pair_local = pairs.shape[0]
    spec_shape = (field_count, 2, pair_local, wave_total + 1)
    rows = SLOTS * (both + 8)
    operands = [pairs, limits, *arrived, *table, *table, *synths, after]
    in_specs = [pl.BlockSpec(memory_space=pl.ANY) for _ in range(8)]
    in_specs += [
        pl.BlockSpec((1, width, wave_total), lambda s, *_: (own, s, 0)) for _ in range(4)
    ]
    in_specs += [
        pl.BlockSpec((1, 16, wave_total), lambda s, *_: (own, SLOTS * width // 16, 0))
        for _ in range(4)
    ]
    in_specs += [
        pl.BlockSpec((1,) + ref.shape[1:], lambda s, *_: (at * SLOTS + s, 0, 0)) for ref in synths
    ]
    in_specs.append(pl.BlockSpec(memory_space=pl.ANY))
    aliases = {}
    if not fresh:
        operands.append(spectrum)
        in_specs.append(pl.BlockSpec(memory_space=pl.ANY))
        aliases = {len(operands) - 1: 0}
    flops = 2 * SLOTS * 4 * both * wave_total * wave_total
    made = pl.pallas_call(
        functools.partial(level_body, at, dims),
        grid_spec=pltpu.PrefetchScalarGridSpec(
            num_scalar_prefetch=2,
            grid=(SLOTS,),
            in_specs=in_specs,
            out_specs=[
                pl.BlockSpec(
                    (field_count, 2, SLOTS, wave_total + 1), lambda s, *_: (0, 0, at, 0)
                ),
            ]
            + [pl.BlockSpec((rows, LANES), lambda s, *_: (0, 0)) for _ in range(8)],
            scratch_shapes=[
                pltpu.VMEM((8,) + arrived[0].shape[1:], BF16),
                pltpu.VMEM((8, rows, LANES), BF16),
                pltpu.SemaphoreType.DMA((8,)),
                pltpu.VMEM((5, field_count * PITCH, LANES), F32),
                pltpu.VMEM((5, field_count * PITCH, LANES), F32),
                pltpu.VMEM((wave_total // LANES + 1, both * SLOTS, LANES), F32),
                pltpu.VMEM((SLOTS * both, 640), BF16),
                pltpu.VMEM((SLOTS * both, 640), BF16),
                pltpu.VMEM((SLOTS * both, LANES), F32),
                pltpu.VMEM((SLOTS * both, LANES), F32),
            ],
        ),
        out_shape=[jax.ShapeDtypeStruct(spec_shape, BF16)]
        + [jax.ShapeDtypeStruct((rows, LANES), BF16)] * 8,
        input_output_aliases=aliases,
        compiler_params=pltpu.CompilerParams(
            dimension_semantics=("arbitrary",), vmem_limit_bytes=VMEM_LIMIT
        ),
        cost_estimate=pl.CostEstimate(
            flops=flops, bytes_accessed=2 * wave_total**2 * SLOTS, transcendentals=0
        ),
        name="levels",
    )(*operands)
    return made[0], made[1:]


def inverse_body(chunks, field_step, lat_ref, *refs):
    arrived = refs[: chunks * 8]
    inv_one, inv_two, inv_three, out_one, out_two, out_three, main, tiny = refs[chunks * 8 :]
    lat = lat_ref[3]
    step = pl.program_id(0)
    both = 2 * out_three.shape[1]
    big = SLOTS * both
    small = SLOTS * 8

    @pl.when(step == 0)
    def _():
        for at in range(chunks):
            for k in range(8):
                place = at * 8 + jnp.bitwise_xor(lat, k)
                part = arrived[at * 8 + k]
                values = part[:big, :].astype(F32)
                for slot in range(SLOTS):
                    start = pl.multiple_of((place * SLOTS + slot) * SPREAD, 8)
                    main[pl.ds(start, both), :] = values[slot * both : (slot + 1) * both]
                tiny[pl.ds(pl.multiple_of(place * small, 16), small), :] = part[big:, :].astype(F32)

    pairs = chunks * 8 * SLOTS
    own = out_one.shape[1]
    turned = []
    for at in range(field_step):
        field = step * field_step + at
        rows = jnp.concatenate(
            [main[pl.ds(c * (both // 2) + field, pairs, stride=SPREAD), :] for c in range(2)], axis=0
        )
        turned.append(rows.T.astype(BF16))
    grid_rows = nn_dot(jnp.concatenate([x[:own] for x in turned], axis=0), inv_one[...])
    for at in range(field_step):
        out_one[at] = grid_rows[at * own : (at + 1) * own]
    rest = LANES - own
    grid_rows = nn_dot(jnp.concatenate([x[own:] for x in turned], axis=0), inv_two[...])
    for at in range(field_step):
        out_two[at] = grid_rows[at * rest : at * rest + out_two.shape[1]]

    @pl.when(step < 4)
    def _():
        for at in range(2):
            inside = 2 * step + at
            rows = tiny[pl.ds(inside, pairs, stride=8), :]
            turned = rows.T.astype(BF16)
            grid_rows = nn_dot(turned[:64], inv_three[:pairs]) + nn_dot(
                turned[64:], inv_three[pairs:]
            )
            count = out_three.shape[0]
            for bundle in range(3):
                for row in range(count):
                    out_three[row, pl.ds(bundle * 8 + inside, 1), :] = grid_rows[
                        bundle * count + row : bundle * count + row + 1
                    ]


def inverse_call(limits, arrived, tables, field_count):
    chunks = len(arrived)
    field_step = 4
    both = 2 * field_count
    whole = lambda shape: pl.BlockSpec(shape, lambda g, *_: (0,) * len(shape))
    flat = [x for parts in arrived for x in parts]
    outs = [(field_count, t.shape[1] // 16, t.shape[1]) for t in tables]
    outs[2] = (outs[2][1], outs[2][0], outs[2][2])
    one, two, three = pl.pallas_call(
        functools.partial(inverse_body, chunks, field_step),
        grid_spec=pltpu.PrefetchScalarGridSpec(
            num_scalar_prefetch=1,
            grid=(field_count // field_step,),
            in_specs=[whole(x.shape) for x in flat] + [whole(t.shape) for t in tables],
            out_specs=[
                pl.BlockSpec((field_step,) + outs[0][1:], lambda g, *_: (g, 0, 0)),
                pl.BlockSpec((field_step,) + outs[1][1:], lambda g, *_: (g, 0, 0)),
                whole(outs[2]),
            ],
            scratch_shapes=[
                pltpu.VMEM((chunks * 8 * SLOTS * SPREAD, LANES), F32),
                pltpu.VMEM((chunks * 8 * SLOTS * 8, LANES), F32),
            ],
        ),
        out_shape=[jax.ShapeDtypeStruct(shape, F32) for shape in outs],
        compiler_params=pltpu.CompilerParams(
            dimension_semantics=("arbitrary",), vmem_limit_bytes=VMEM_LIMIT
        ),
        cost_estimate=pl.CostEstimate(
            flops=2 * field_count * LANES * both * 640, bytes_accessed=1 << 24, transcendentals=0
        ),
        name="inverse",
    )(limits, *flat, *tables)
    return one, two, three.transpose(1, 0, 2)


def chunked_on_device(grid_fields, assign, limits, legendre, synth_one, synth_two, synth_three):
    lat_count = lax.axis_size("lat")
    field_count, row_count, _ = grid_fields.shape
    pair_total = assign.shape[0]
    pair_local = pair_total // lat_count
    wave_total = 2 * pair_total
    chunks = pair_local // SLOTS
    synths = (synth_one, synth_two, synth_three)
    lat = lax.axis_index("lat").astype(jnp.int32)
    by_owner = assign.reshape(lat_count, chunks, SLOTS)
    own_pairs = lax.dynamic_slice(assign, (lat * pair_local,), (pair_local,))
    south = (lat >= lat_count // 2).astype(jnp.int32)
    small = row_count - LANES
    shift = jnp.stack([south * small, (1 - south) * LANES])

    here = lax.axis_index("fld").astype(jnp.int32)
    scalars = jnp.concatenate([limits, jnp.stack([lat, here])])
    partners = jnp.bitwise_xor(lat, jnp.arange(lat_count, dtype=jnp.int32))
    to_partner = jnp.take(by_owner, partners, axis=0).astype(F32)
    turned = legendre.transpose(0, 2, 1)
    waves = jnp.stack([to_partner, wave_total - 1 - to_partner], axis=3)
    waves = waves.transpose(1, 0, 2, 3).reshape(1, -1)
    per_chunk = lat_count * 2 * SLOTS

    def exchange(parts):
        return [parts[0]] + [
            lax.ppermute(parts[k], "lat", [(i, i ^ k) for i in range(lat_count)])
            for k in range(1, lat_count)
        ]

    def across(value, k):
        return lax.ppermute(value, "fld", [(i, i ^ k) for i in range(4)])

    def gather(first, last, after):
        packed = turn_call(first, last, turned, after)
        far = across(packed, 2)
        table = [packed, across(packed, 1), far, across(far, 1)]
        return [(table, piece) for piece in range(last - first)]

    def transform(first, groups, after):
        total = sum(groups)
        span = waves[:, first * per_chunk : (first + total) * per_chunk]
        sent = dft_call(groups, shift, span, grid_fields, after)
        for place, size in enumerate(groups):
            moved = exchange(sent[place])
            crossed.extend((moved, piece) for piece in range(size))
        return sent[0][0]

    order = by_owner.transpose(1, 0, 2).reshape(-1)
    lengths = [4 * table.shape[1] for table in synths]
    crossed, spectrum, arrived = [], None, []
    head = transform(0, (1,), assign)
    tables = gather(0, 1, head)
    inverses = None
    middle = min(3, chunks)
    for at in range(chunks):
        if at == 0 and chunks > 1:
            head = transform(1, (middle - 1,), tables[0][0][0])
            tables += gather(1, middle, head)
        (moved, piece), (table, own) = crossed[at], tables[at]
        spectrum, send = level_call(
            at, piece, own, own_pairs, scalars, moved, table, synths, head, spectrum, field_count
        )
        arrived.append(exchange(send))
        if at == 0:
            if chunks > middle:
                head = transform(middle, (1,) * (chunks - middle), send[0])
                tables += gather(middle, chunks, head)
            inverses = tables_call(order, lengths, head)
            head = inverses[0]
    return (spectrum, *inverse_call(scalars, arrived, inverses, field_count))


def on_device(*arguments):
    if fits(*arguments):
        return chunked_on_device(*arguments)
    return plain_on_device(*arguments)


def solution(mesh):
    return jax.shard_map(
        on_device,
        mesh=mesh,
        in_specs=(
            P("fld", "lat", None),
            P(),
            P(),
            P("lat", None, "fld"),
            P("lat", None, None),
            P("lat", None, None),
            P("lat", None, None),
        ),
        out_specs=(
            P("fld", None, "lat", None),
            P("fld", "lat", None),
            P("fld", "lat", None),
            P("fld", "lat", None),
        ),
        check_vma=False,
    )
```
